32 devices in a mesh: sec: 16 (over z, y, x), tile: 2 (over core).
Axes of the slice: x: 2, y: 2, z: 4, core: 2. Of those that a mesh axis runs over, the one named last changes fastest.
Arguments:
- image: bfloat16 [16, 512, 384], P('sec', 'tile'), may hold values from -12 to 12
- field: float32 [16, 2, 512, 384], P('sec', None, 'tile'), may hold values from -1.5 to 1.5
- displacement: int32 [4, 16, 2, 2], replicated, may hold values from -1 to 1
Outputs:
- aligned: float32 [16, 2, 512, 384], P('sec', None, 'tile')
The draws below stay inside these ranges and needn't reach their ends.
All inputs are finite; a program needn't handle non-finite values.
Results may differ from the reference program's by a relative error of at most 0.01.
The reference program's roundings to bfloat16 on the way (of `warped`) count: a program that leaves them out, or rounds other values in their place, can miss the bound.
Values may be sent and summed in bfloat16 or wider, within the bound.
A program may use at most 64 MiB of HBM per device.

```python
import jax
import jax.numpy as jnp
from jax import lax

WIDTH = 384
BLOCK = 128
ITERS = 4
SECTIONS = 16
HEIGHT = 512


def draw_image(key, part):
    shape = (SECTIONS, HEIGHT, WIDTH)
    scales = 1.0 + 2.0 * jnp.arange(SECTIONS, dtype=jnp.float32) / (SECTIONS - 1)
    values = jax.random.truncated_normal(key, -4.0, 4.0, shape, jnp.float32)
    return (values * scales[:, None, None]).astype(jnp.bfloat16)


def touch_ends(entries, rng, smallest, top_value):
    extent = entries.shape
    place = [jax.random.randint(jax.random.fold_in(rng, axis), (), 0, extent[axis]) for axis in range(len(extent))]
    entries = entries.at[tuple(place)].set(smallest)
    longest = extent.index(max(extent))
    place[longest] = (place[longest] + 1) % extent[longest]
    return entries.at[tuple(place)].set(top_value)


def shard_levels(stream_key, extent, shards, least, largest):
    factor_of, own = 1.0, jax.random.fold_in(stream_key, 6)
    for axis_at, parts in shards:
        steps = jnp.exp(jax.random.uniform(jax.random.fold_in(own, axis_at), (parts,), jnp.float32, least / len(shards), largest / len(shards)))
        factor_of = factor_of * jnp.repeat(steps, extent[axis_at] // parts).reshape([-1 if axis == axis_at else 1 for axis in range(len(extent))])
    return factor_of


def gaussian(own_key, dims, deviation, bound, pieces=(), held_as=jnp.bfloat16):
    entries = deviation * jax.random.normal(own_key, dims, jnp.float32)
    if pieces:
        entries = entries * shard_levels(own_key, dims, pieces, -0.22, 0.18)
    return jnp.clip(entries, -bound, bound).astype(held_as)


def setup_inputs(seed: int = 0) -> dict:
    key_list = jax.random.split(jax.random.key(seed), 4)
    return {
        "image": draw_image(jax.random.fold_in(key_list[3], 71), 0),
        "field": gaussian(key_list[1], (SECTIONS, 2, HEIGHT, WIDTH), 0.3, 1.5, ((0, 16), (2, 2)), jnp.float32),
        "displacement": touch_ends(jax.random.randint(key_list[2], (ITERS, SECTIONS, 2, 2), -1, 2), jax.random.fold_in(key_list[2], 1), -1, 1).astype(jnp.int32),
    }


charb_eps2 = 0.25
step_size = 0.2
smooth_weight = 0.5

def block_move(planes, rows_by, cols_by):
    height = planes.shape[1]
    width = planes.shape[2]

    def single(plane, down, across):
        padded = jnp.pad(plane, ((BLOCK, BLOCK), (BLOCK, BLOCK)))
        return lax.dynamic_slice(padded, ((BLOCK + BLOCK * down).astype(jnp.int32), (BLOCK + BLOCK * across).astype(jnp.int32)), (height, width))
    return jax.vmap(single)(planes, rows_by, cols_by)

def inside(rows_by, cols_by, height, width):
    row_pos = jnp.arange(height, dtype=jnp.int32)[None, :] + BLOCK * rows_by[:, None]
    col_pos = jnp.arange(width, dtype=jnp.int32)[None, :] + BLOCK * cols_by[:, None]
    good_rows = ((row_pos >= 0) & (row_pos < height)).astype(jnp.float32)
    good_cols = ((col_pos >= 0) & (col_pos < width)).astype(jnp.float32)
    return good_rows[:, :, None] * good_cols[:, None, :]

def reference(image, field, displacement):
    sections, height, width = image.shape
    plane = image.astype(jnp.float32)
    padded = jnp.pad(plane, ((0, 0), (1, 1), (1, 1)))
    grad_rows = 0.5 * (padded[:, 2:, 1:-1] - padded[:, :-2, 1:-1])
    grad_cols = 0.5 * (padded[:, 1:-1, 2:] - padded[:, 1:-1, :-2])
    current = field
    section_ids = jnp.arange(sections, dtype=jnp.int32)
    for turn in range(ITERS):
        warped = (plane + grad_rows * current[:, 0] + grad_cols * current[:, 1]).astype(jnp.bfloat16)
        values = warped.astype(jnp.float32)
        combined = jnp.zeros((sections, height, width), jnp.float32)
        energy = jnp.zeros((), jnp.float32)
        count = jnp.zeros((), jnp.int32)
        for spacing in (1, 2):
            rows_by = displacement[turn, :, spacing - 1, 0]
            cols_by = displacement[turn, :, spacing - 1, 1]
            exists = section_ids + spacing < sections
            partner = jnp.concatenate([values[spacing:], jnp.zeros((spacing, height, width), jnp.float32)], axis=0)
            moved = block_move(partner, rows_by, cols_by)
            mask = inside(rows_by, cols_by, height, width) * exists.astype(jnp.float32)[:, None, None]
            resid = mask * (values - moved)
            scaled = resid / jnp.sqrt(resid * resid + charb_eps2)
            energy = energy + jnp.sum(scaled * resid)
            count = count + jnp.sum(exists.astype(jnp.int32) * (height - BLOCK * jnp.abs(rows_by)) * (width - BLOCK * jnp.abs(cols_by)))
            earlier = jnp.concatenate([jnp.zeros((spacing, height, width), jnp.float32), scaled[:-spacing]], axis=0)
            earlier_rows = jnp.concatenate([jnp.zeros((spacing,), jnp.int32), rows_by[:-spacing]], axis=0)
            earlier_cols = jnp.concatenate([jnp.zeros((spacing,), jnp.int32), cols_by[:-spacing]], axis=0)
            back = block_move(earlier, -earlier_rows, -earlier_cols)
            combined = combined + (scaled - back)
        factor = step_size / (1.0 + energy / count.astype(jnp.float32))
        field_pad = jnp.pad(current, ((0, 0), (0, 0), (1, 1), (1, 1)))
        neighbours = field_pad[:, :, 2:, 1:-1] + field_pad[:, :, :-2, 1:-1] + (field_pad[:, :, 1:-1, 2:] + field_pad[:, :, 1:-1, :-2])
        data_term = jnp.stack([combined * grad_rows, combined * grad_cols], axis=1)
        current = current - factor * (data_term + smooth_weight * (4.0 * current - neighbours))
    return current
```

```python
import functools

import jax
import jax.numpy as jnp
from jax import lax
from jax.experimental import pallas as pl
from jax.experimental.pallas import tpu as pltpu
from jax.sharding import PartitionSpec as P

BLOCK = 128
ITERS = 4
CHUNK = 32
PAD = 8
OFFSETS = (1, 2, -1, -2)

charb_eps2 = 0.25
step_size = 0.2
smooth_weight = 0.5

MESH = pl.DeviceIdType.MESH


def kernel(sections, tiles, image_ref, field_ref, disp_ref, out_ref, *scratch):
    moved_refs = (scratch[0:4], scratch[4:8])
    (warp_ref, u_ref, img_ref, grow_ref, gcol_ref, comb_ref, data_ref, own_ref, sum_ref, tile_slots, sec_slots) = scratch[8:19]
    (img_send, img_recv, u_send, u_recv, w_send, w_recv, h_send, h_recv, t_send, t_recv, s_send, s_recv) = scratch[19:]
    rows, width = grow_ref.shape
    height = rows * tiles
    cols = width // BLOCK
    chunks = rows // CHUNK
    section = lax.axis_index("sec")
    tile = lax.axis_index("tile")

    barrier = pltpu.get_barrier_semaphore()
    for d in range(1, sections):
        pl.semaphore_signal(barrier, inc=1, device_id=(lax.rem(section + d, sections), tile), device_id_type=MESH)
    for d in range(1, tiles):
        pl.semaphore_signal(barrier, inc=1, device_id=(section, lax.rem(tile + d, tiles)), device_id_type=MESH)

    def remote(src, dst, send, recv, sec_at, tile_at):
        return pltpu.make_async_remote_copy(
            src_ref=src, dst_ref=dst, send_sem=send, recv_sem=recv, device_id=(sec_at, tile_at), device_id_type=MESH
        )

    has_above = tile > 0
    has_below = tile < tiles - 1
    above = jnp.maximum(tile - 1, 0)
    below = jnp.minimum(tile + 1, tiles - 1)

    def edge_copies(ref, send, recv):
        up = remote(ref.at[..., pl.ds(PAD, PAD), :], ref.at[..., pl.ds(rows + PAD, PAD), :], send.at[0], recv.at[0], section, above)
        down = remote(ref.at[..., pl.ds(rows, PAD), :], ref.at[..., pl.ds(0, PAD), :], send.at[1], recv.at[1], section, below)
        return up, down

    def edge_start(ref, send, recv):
        up, down = edge_copies(ref, send, recv)
        pl.when(has_above)(up.start)
        pl.when(has_below)(down.start)

    def edge_wait(ref, send, recv):
        up, down = edge_copies(ref, send, recv)
        pl.when(has_below)(up.wait_recv)
        pl.when(has_above)(down.wait_recv)
        pl.when(has_above)(up.wait_send)
        pl.when(has_below)(down.wait_send)

    @pl.when(jnp.logical_not(has_above))
    def _():
        img_ref[0:PAD, :] = jnp.zeros((PAD, width), jnp.float32)
        for p in range(2):
            u_ref[p, :, 0:PAD, :] = jnp.zeros((2, PAD, width), jnp.float32)

    @pl.when(jnp.logical_not(has_below))
    def _():
        img_ref[rows + PAD : rows + 2 * PAD, :] = jnp.zeros((PAD, width), jnp.float32)
        for p in range(2):
            u_ref[p, :, rows + PAD : rows + 2 * PAD, :] = jnp.zeros((2, PAD, width), jnp.float32)

    def chunk_loop(body, init=None):
        def step(c, carry):
            return body(c, pl.multiple_of(c * CHUNK, CHUNK), carry)

        return lax.fori_loop(0, chunks, step, init)

    def load_in(c, r, carry):
        img_ref[pl.ds(r + PAD, CHUNK), :] = image_ref[0, pl.ds(r, CHUNK), :].astype(jnp.float32)
        u_ref[0, :, pl.ds(r + PAD, CHUNK), :] = field_ref[0, :, pl.ds(r, CHUNK), :]
        return carry

    chunk_loop(load_in, 0)

    pl.semaphore_wait(barrier, sections - 1 + tiles - 1)
    edge_start(img_ref, img_send, img_recv)
    edge_wait(img_ref, img_send, img_recv)

    def block_of(c):
        block = c // (BLOCK // CHUNK)
        return block, pl.multiple_of((c - block * (BLOCK // CHUNK)) * CHUNK, CHUNK)

    col_ids = lax.broadcasted_iota(jnp.int32, (CHUNK, width), 1)

    def left_right(x):
        left = jnp.where(col_ids == 0, 0.0, pltpu.roll(x, 1, 1))
        right = jnp.where(col_ids == width - 1, 0.0, pltpu.roll(x, width - 1, 1))
        return left, right

    def store_warp(p, c, base, grow, gcol, u0, u1):
        warped = (base + grow * u0 + gcol * u1).astype(jnp.bfloat16)
        block, sub = block_of(c)
        for j in range(cols):
            warp_ref[p, block, j, pl.ds(sub, CHUNK), :] = warped[:, j * BLOCK : (j + 1) * BLOCK]

    def first_warp(c, r, carry):
        band = img_ref[pl.ds(r, CHUNK + 2 * PAD), :]
        base = band[PAD : PAD + CHUNK]
        grow = 0.5 * (band[PAD + 1 : PAD + 1 + CHUNK] - band[PAD - 1 : PAD - 1 + CHUNK])
        left, right = left_right(base)
        gcol = 0.5 * (right - left)
        grow_ref[pl.ds(r, CHUNK), :] = grow
        gcol_ref[pl.ds(r, CHUNK), :] = gcol
        u0 = u_ref[0, 0, pl.ds(r + PAD, CHUNK), :]
        u1 = u_ref[0, 1, pl.ds(r + PAD, CHUNK), :]
        store_warp(0, c, base, grow, gcol, u0, u1)
        return carry

    chunk_loop(first_warp, 0)

    def in_stack(at):
        return (at >= 0) & (at < sections)

    def step(turn, p):
        refs = moved_refs[p]

        def main_copy(i):
            target = jnp.clip(section - OFFSETS[i], 0, sections - 1)
            return remote(
                warp_ref.at[p], refs[i].at[pl.ds(1, rows // BLOCK)], w_send.at[p, i], w_recv.at[p, i], target, tile
            )

        def relay_up(i):
            return remote(
                refs[i].at[1], refs[i].at[rows // BLOCK + 1],
                h_send.at[p, i, 0], h_recv.at[p, i, 0], section, above,
            )

        def relay_down(i):
            return remote(
                refs[i].at[rows // BLOCK], refs[i].at[0],
                h_send.at[p, i, 1], h_recv.at[p, i, 1], section, below,
            )

        def start_main(i):
            pl.when(in_stack(section - OFFSETS[i]))(main_copy(i).start)

        def relay(i):
            @pl.when(in_stack(section + OFFSETS[i]))
            def _():
                main_copy(i).wait_recv()
                pl.when(has_above)(relay_up(i).start)
                pl.when(has_below)(relay_down(i).start)

        def arrive(i):
            @pl.when(in_stack(section + OFFSETS[i]))
            def _():
                pl.when(has_below)(relay_up(i).wait_recv)
                pl.when(has_above)(relay_down(i).wait_recv)

        def finish(i):
            pl.when(in_stack(section - OFFSETS[i]))(main_copy(i).wait_send)

            @pl.when(in_stack(section + OFFSETS[i]))
            def _():
                pl.when(has_above)(relay_up(i).wait_send)
                pl.when(has_below)(relay_down(i).wait_send)

        for i in range(4):
            start_main(i)
        edge_start(u_ref.at[p], u_send.at[p], u_recv.at[p])

        def count_one(s, total):
            for g in (1, 2):
                at = ((turn * sections + s) * 2 + (g - 1)) * 2
                area = (height - BLOCK * jnp.abs(disp_ref[at])) * (width - BLOCK * jnp.abs(disp_ref[at + 1]))
                total = total + (s + g < sections).astype(jnp.int32) * area
            return total

        count = lax.fori_loop(0, sections, count_one, jnp.int32(0))

        def shift_of(i):
            g = abs(OFFSETS[i])
            first = section if OFFSETS[i] > 0 else jnp.maximum(section - g, 0)
            sign = 1 if OFFSETS[i] > 0 else -1
            at = ((turn * sections + first) * 2 + (g - 1)) * 2
            return sign * disp_ref[at], sign * disp_ref[at + 1]

        def residual(i, c, r, j, own, down, across):
            block, sub = block_of(c)
            row_block = tile * (rows // BLOCK) + block + down
            col_block = j + across
            good = in_stack(section + OFFSETS[i]) & (row_block >= 0) & (row_block < height // BLOCK)
            good = good & (col_block >= 0) & (col_block < cols)
            other = refs[i][block + 1 + down, jnp.minimum(jnp.maximum(col_block, 0), cols - 1), pl.ds(sub, CHUNK), :].astype(jnp.float32)
            mask = jnp.full((CHUNK, BLOCK), good.astype(jnp.int32), jnp.int32)
            resid = jnp.where(mask > 0, own - other, 0.0)
            return resid, resid * lax.rsqrt(resid * resid + charb_eps2)

        relay(0)
        relay(1)
        arrive(0)
        arrive(1)
        shifts = [shift_of(i) for i in range(4)]

        def forward(c, r, energy):
            block, sub = block_of(c)
            for j in range(cols):
                own = warp_ref[p, block, j, pl.ds(sub, CHUNK), :].astype(jnp.float32)
                resid_a, scaled_a = residual(0, c, r, j, own, *shifts[0])
                resid_b, scaled_b = residual(1, c, r, j, own, *shifts[1])
                energy = energy + (resid_a * scaled_a + resid_b * scaled_b)
                comb_ref[pl.ds(r, CHUNK), j * BLOCK : (j + 1) * BLOCK] = scaled_a + scaled_b
            return energy

        energy = chunk_loop(forward, jnp.zeros((CHUNK, BLOCK), jnp.float32))
        own_ref[p] = jnp.sum(energy.reshape(CHUNK // 8, 8, BLOCK), axis=0)

        def tile_copy(d):
            return remote(own_ref.at[p], tile_slots.at[p, d - 1], t_send.at[p, d - 1], t_recv.at[p, d - 1], section, lax.rem(tile + d, tiles))

        def sec_copy(d):
            return remote(sum_ref.at[p], sec_slots.at[p, d - 1], s_send.at[p, d - 1], s_recv.at[p, d - 1], lax.rem(section + d, sections), tile)

        for d in range(1, tiles):
            tile_copy(d).start()
        relay(2)
        relay(3)
        total = own_ref[p]
        for d in range(1, tiles):
            tile_copy(d).wait_recv()
            total = total + tile_slots[p, d - 1]
        sum_ref[p] = total
        for d in range(1, sections):
            sec_copy(d).start()
        arrive(2)
        arrive(3)
        edge_wait(u_ref.at[p], u_send.at[p], u_recv.at[p])

        def backward(c, r, carry):
            block, sub = block_of(c)
            parts = []
            for j in range(cols):
                own = warp_ref[p, block, j, pl.ds(sub, CHUNK), :].astype(jnp.float32)
                _, scaled_a = residual(2, c, r, j, own, *shifts[2])
                _, scaled_b = residual(3, c, r, j, own, *shifts[3])
                parts.append(comb_ref[pl.ds(r, CHUNK), j * BLOCK : (j + 1) * BLOCK] + (scaled_a + scaled_b))
            combined = jnp.concatenate(parts, axis=1)
            for n, grad_ref in enumerate((grow_ref, gcol_ref)):
                band = u_ref[p, n, pl.ds(r, CHUNK + 2 * PAD), :]
                here = band[PAD : PAD + CHUNK]
                left, right = left_right(here)
                around = band[PAD + 1 : PAD + 1 + CHUNK] + band[PAD - 1 : PAD - 1 + CHUNK] + (right + left)
                data_ref[n, pl.ds(r, CHUNK), :] = combined * grad_ref[pl.ds(r, CHUNK), :] + smooth_weight * (4.0 * here - around)
            return carry

        chunk_loop(backward, 0)

        for i in range(4):
            finish(i)
        total = sum_ref[p]
        for d in range(1, sections):
            sec_copy(d).wait_recv()
            total = total + sec_slots[p, d - 1]
        energy_all = jnp.sum(jnp.sum(total, axis=0, keepdims=True), axis=1, keepdims=True)
        count_all = jnp.full((1, 1), count, jnp.int32).astype(jnp.float32)
        factor = step_size / (1.0 + energy_all / count_all)
        for d in range(1, tiles):
            tile_copy(d).wait_send()
        for d in range(1, sections):
            sec_copy(d).wait_send()

        def update(c, r, carry):
            news = []
            for n in range(2):
                new = u_ref[p, n, pl.ds(r + PAD, CHUNK), :] - factor * data_ref[n, pl.ds(r, CHUNK), :]
                u_ref[1 - p, n, pl.ds(r + PAD, CHUNK), :] = new
                news.append(new)
            base = img_ref[pl.ds(r + PAD, CHUNK), :]
            store_warp(1 - p, c, base, grow_ref[pl.ds(r, CHUNK), :], gcol_ref[pl.ds(r, CHUNK), :], *news)
            return carry

        chunk_loop(update, 0)

    def two_steps(half, carry):
        step(2 * half, 0)
        step(2 * half + 1, 1)
        return carry

    lax.fori_loop(0, ITERS // 2, two_steps, 0)

    def store_out(c, r, carry):
        out_ref[0, :, pl.ds(r, CHUNK), :] = u_ref[0, :, pl.ds(r + PAD, CHUNK), :]
        return carry

    chunk_loop(store_out, 0)


def solution(mesh):
    sections, tiles = mesh.shape["sec"], mesh.shape["tile"]

    def per_device(image, field, displacement):
        rows, width = image.shape[1], image.shape[2]
        cols = width // BLOCK
        dma = pltpu.SemaphoreType.DMA
        return pl.pallas_call(
            functools.partial(kernel, sections, tiles),
            out_shape=jax.ShapeDtypeStruct(field.shape, jnp.float32),
            in_specs=[
                pl.BlockSpec(memory_space=pltpu.VMEM),
                pl.BlockSpec(memory_space=pltpu.VMEM),
                pl.BlockSpec(memory_space=pltpu.SMEM),
            ],
            out_specs=pl.BlockSpec(memory_space=pltpu.VMEM),
            scratch_shapes=[pltpu.VMEM((rows // BLOCK + 2, cols, BLOCK, BLOCK), jnp.bfloat16) for _ in range(8)]
            + [
                pltpu.VMEM((2, rows // BLOCK, cols, BLOCK, BLOCK), jnp.bfloat16),
                pltpu.VMEM((2, 2, rows + 2 * PAD, width), jnp.float32),
                pltpu.VMEM((rows + 2 * PAD, width), jnp.float32),
                pltpu.VMEM((rows, width), jnp.float32),
                pltpu.VMEM((rows, width), jnp.float32),
                pltpu.VMEM((rows, width), jnp.float32),
                pltpu.VMEM((2, rows, width), jnp.float32),
                pltpu.VMEM((2, 8, BLOCK), jnp.float32),
                pltpu.VMEM((2, 8, BLOCK), jnp.float32),
                pltpu.VMEM((2, tiles - 1, 8, BLOCK), jnp.float32),
                pltpu.VMEM((2, sections - 1, 8, BLOCK), jnp.float32),
                dma((2,)), dma((2,)),
                dma((2, 2)), dma((2, 2)),
                dma((2, 4)), dma((2, 4)),
                dma((2, 4, 2)), dma((2, 4, 2)),
                dma((2, tiles - 1)), dma((2, tiles - 1)),
                dma((2, sections - 1)), dma((2, sections - 1)),
            ],
            compiler_params=pltpu.CompilerParams(
                collective_id=0, has_side_effects=True, vmem_limit_bytes=48 * 1024 * 1024
            ),
        )(image, field, displacement.reshape(-1))

    return jax.shard_map(
        per_device,
        mesh=mesh,
        in_specs=(P("sec", "tile", None), P("sec", None, "tile", None), P()),
        out_specs=P("sec", None, "tile", None),
        check_vma=False,
    )
```

```python
import functools

import jax
import jax.numpy as jnp
from jax import lax
from jax.experimental import pallas as pl
from jax.experimental.pallas import tpu as pltpu
from jax.sharding import PartitionSpec as P

BLOCK = 128
ITERS = 4
CHUNK = 32
PAD = 8
OFFSETS = (1, 2, -1, -2)
EXTRA = 4

GROUP = (
    (((1, 2), (2, 3), (-4, EXTRA)), (0, 1, EXTRA), (2, 3), {0: (2, 2), 1: (4, 3), EXTRA: (3, 0)}),
    (((-1, 0), (2, 3)), (1, 2), (0, 3), {1: (4, 3)}),
    (((1, 2), (-2, 1)), (0, 3), (2, 1), {3: (-4, 1)}),
    (((-1, 0), (-2, 1), (4, EXTRA)), (2, 3, EXTRA), (0, 1), {2: (-2, 0), 3: (-4, 1), EXTRA: (-3, 2)}),
)
DIRECT = ((((-1, 0), (-2, 1), (1, 2), (2, 3)), (0, 1, 2, 3), (), {}),)

charb_eps2 = 0.25
step_size = 0.2
smooth_weight = 0.5

MESH = pl.DeviceIdType.MESH


def kernel(sections, tiles, image_ref, field_ref, disp_ref, out_ref, *scratch):
    moved_refs = (scratch[0:5], scratch[5:10])
    (warp_ref, u_ref, img_ref, grow_ref, gcol_ref, comb_ref, data_ref, own_ref, sum_ref, tile_slots, sec_slots) = scratch[10:21]
    (img_send, img_recv, u_send, u_recv, w_send, w_recv, h_send, h_recv, r_send, t_send, t_recv, s_send, s_recv) = scratch[21:]
    rows, width = grow_ref.shape
    height = rows * tiles
    cols = width // BLOCK
    chunks = rows // CHUNK
    pieces = rows // BLOCK
    plan = GROUP if sections % len(GROUP) == 0 else DIRECT
    section = lax.axis_index("sec")
    tile = lax.axis_index("tile")

    barrier = pltpu.get_barrier_semaphore()
    for d in range(1, sections):
        pl.semaphore_signal(barrier, inc=1, device_id=(lax.rem(section + d, sections), tile), device_id_type=MESH)
    for d in range(1, tiles):
        pl.semaphore_signal(barrier, inc=1, device_id=(section, lax.rem(tile + d, tiles)), device_id_type=MESH)

    def remote(src, dst, send, recv, sec_at, tile_at):
        return pltpu.make_async_remote_copy(
            src_ref=src, dst_ref=dst, send_sem=send, recv_sem=recv, device_id=(sec_at, tile_at), device_id_type=MESH
        )

    has_above = tile > 0
    has_below = tile < tiles - 1
    above = jnp.maximum(tile - 1, 0)
    below = jnp.minimum(tile + 1, tiles - 1)

    def edge_copies(ref, send, recv):
        up = remote(ref.at[..., pl.ds(PAD, PAD), :], ref.at[..., pl.ds(rows + PAD, PAD), :], send.at[0], recv.at[0], section, above)
        down = remote(ref.at[..., pl.ds(rows, PAD), :], ref.at[..., pl.ds(0, PAD), :], send.at[1], recv.at[1], section, below)
        return up, down

    def edge_start(ref, send, recv):
        up, down = edge_copies(ref, send, recv)
        pl.when(has_above)(up.start)
        pl.when(has_below)(down.start)

    def edge_wait(ref, send, recv):
        up, down = edge_copies(ref, send, recv)
        pl.when(has_below)(up.wait_recv)
        pl.when(has_above)(down.wait_recv)
        pl.when(has_above)(up.wait_send)
        pl.when(has_below)(down.wait_send)

    @pl.when(jnp.logical_not(has_above))
    def _():
        img_ref[0:PAD, :] = jnp.zeros((PAD, width), jnp.float32)
        for p in range(2):
            u_ref[p, :, 0:PAD, :] = jnp.zeros((2, PAD, width), jnp.float32)

    @pl.when(jnp.logical_not(has_below))
    def _():
        img_ref[rows + PAD : rows + 2 * PAD, :] = jnp.zeros((PAD, width), jnp.float32)
        for p in range(2):
            u_ref[p, :, rows + PAD : rows + 2 * PAD, :] = jnp.zeros((2, PAD, width), jnp.float32)

    def chunk_loop(body, init=None):
        def step(c, carry):
            return body(c, pl.multiple_of(c * CHUNK, CHUNK), carry)

        return lax.fori_loop(0, chunks, step, init)

    def load_in(c, r, carry):
        img_ref[pl.ds(r + PAD, CHUNK), :] = image_ref[0, pl.ds(r, CHUNK), :].astype(jnp.float32)
        u_ref[0, :, pl.ds(r + PAD, CHUNK), :] = field_ref[0, :, pl.ds(r, CHUNK), :]
        return carry

    chunk_loop(load_in, 0)

    pl.semaphore_wait(barrier, sections - 1 + tiles - 1)
    edge_start(img_ref, img_send, img_recv)
    edge_wait(img_ref, img_send, img_recv)

    def block_of(c):
        block = c // (BLOCK // CHUNK)
        return block, pl.multiple_of((c - block * (BLOCK // CHUNK)) * CHUNK, CHUNK)

    col_ids = lax.broadcasted_iota(jnp.int32, (CHUNK, width), 1)

    def left_right(x):
        left = jnp.where(col_ids == 0, 0.0, pltpu.roll(x, 1, 1))
        right = jnp.where(col_ids == width - 1, 0.0, pltpu.roll(x, width - 1, 1))
        return left, right

    def store_warp(p, c, base, grow, gcol, u0, u1):
        warped = (base + grow * u0 + gcol * u1).astype(jnp.bfloat16)
        block, sub = block_of(c)
        for j in range(cols):
            warp_ref[p, block, j, pl.ds(sub, CHUNK), :] = warped[:, j * BLOCK : (j + 1) * BLOCK]

    def first_warp(c, r, carry):
        band = img_ref[pl.ds(r, CHUNK + 2 * PAD), :]
        base = band[PAD : PAD + CHUNK]
        grow = 0.5 * (band[PAD + 1 : PAD + 1 + CHUNK] - band[PAD - 1 : PAD - 1 + CHUNK])
        left, right = left_right(base)
        gcol = 0.5 * (right - left)
        grow_ref[pl.ds(r, CHUNK), :] = grow
        gcol_ref[pl.ds(r, CHUNK), :] = gcol
        u0 = u_ref[0, 0, pl.ds(r + PAD, CHUNK), :]
        u1 = u_ref[0, 1, pl.ds(r + PAD, CHUNK), :]
        store_warp(0, c, base, grow, gcol, u0, u1)
        return carry

    chunk_loop(first_warp, 0)

    def in_stack(at):
        return (at >= 0) & (at < sections)

    def step(turn, p):
        refs = moved_refs[p]

        def source_of(place, i):
            return OFFSETS[i] if i != EXTRA else (4 if place == 0 else -4)

        def piece_copy(src, slot, q, send, offset):
            target = jnp.minimum(jnp.maximum(section + offset, 0), sections - 1)
            return remote(src, refs[slot].at[1 + q], send, w_recv.at[p, slot, q], target, tile)

        def own_copy(offset, slot, q):
            return piece_copy(warp_ref.at[p, q], slot, q, w_send.at[p, slot, q], offset)

        def pass_copy(i, offset, slot, q):
            return piece_copy(refs[i].at[1 + q], slot, q, r_send.at[p, i, q], offset)

        def relay_up(i):
            return remote(
                refs[i].at[1], refs[i].at[rows // BLOCK + 1],
                h_send.at[p, i, 0], h_recv.at[p, i, 0], section, above,
            )

        def relay_down(i):
            return remote(
                refs[i].at[rows // BLOCK], refs[i].at[0],
                h_send.at[p, i, 1], h_recv.at[p, i, 1], section, below,
            )

        def start_own(place):
            for q in range(pieces):
                for offset, slot in plan[place][0]:
                    pl.when(in_stack(section + offset))(own_copy(offset, slot, q).start)

        def receive(place):
            _, near, far, passes = plan[place]
            for slots in (near, far):
                for q in range(pieces):
                    for i in slots:

                        @pl.when(in_stack(section + source_of(place, i)))
                        def _():
                            own_copy(0, i, q).wait_recv()
                            if i in passes:
                                offset, slot = passes[i]
                                pl.when(in_stack(section + offset))(pass_copy(i, offset, slot, q).start)
                            if i != EXTRA and q == 0:
                                pl.when(has_above)(relay_up(i).start)
                            if i != EXTRA and q == pieces - 1:
                                pl.when(has_below)(relay_down(i).start)

        def arrive(i):
            @pl.when(in_stack(section + OFFSETS[i]))
            def _():
                pl.when(has_below)(relay_up(i).wait_recv)
                pl.when(has_above)(relay_down(i).wait_recv)

        def finish(place):
            own, _, _, passes = plan[place]
            for q in range(pieces):
                for offset, slot in own:
                    pl.when(in_stack(section + offset))(own_copy(offset, slot, q).wait_send)
                for i, (offset, slot) in passes.items():
                    has_both = in_stack(section + source_of(place, i)) & in_stack(section + offset)
                    pl.when(has_both)(pass_copy(i, offset, slot, q).wait_send)

        def finish_relay(i):
            @pl.when(in_stack(section + OFFSETS[i]))
            def _():
                pl.when(has_above)(relay_up(i).wait_send)
                pl.when(has_below)(relay_down(i).wait_send)

        def each_place(action):
            for place in range(len(plan)):
                pl.when(lax.rem(section, len(plan)) == place)(functools.partial(action, place))

        each_place(start_own)
        edge_start(u_ref.at[p], u_send.at[p], u_recv.at[p])

        def count_one(s, total):
            for g in (1, 2):
                at = ((turn * sections + s) * 2 + (g - 1)) * 2
                area = (height - BLOCK * jnp.abs(disp_ref[at])) * (width - BLOCK * jnp.abs(disp_ref[at + 1]))
                total = total + (s + g < sections).astype(jnp.int32) * area
            return total

        count = lax.fori_loop(0, sections, count_one, jnp.int32(0))

        def shift_of(i):
            g = abs(OFFSETS[i])
            first = section if OFFSETS[i] > 0 else jnp.maximum(section - g, 0)
            sign = 1 if OFFSETS[i] > 0 else -1
            at = ((turn * sections + first) * 2 + (g - 1)) * 2
            return sign * disp_ref[at], sign * disp_ref[at + 1]

        def residual(i, c, r, j, own, down, across):
            block, sub = block_of(c)
            row_block = tile * (rows // BLOCK) + block + down
            col_block = j + across
            good = in_stack(section + OFFSETS[i]) & (row_block >= 0) & (row_block < height // BLOCK)
            good = good & (col_block >= 0) & (col_block < cols)
            other = refs[i][block + 1 + down, jnp.minimum(jnp.maximum(col_block, 0), cols - 1), pl.ds(sub, CHUNK), :].astype(jnp.float32)
            mask = jnp.full((CHUNK, BLOCK), good.astype(jnp.int32), jnp.int32)
            resid = jnp.where(mask > 0, own - other, 0.0)
            return resid, resid * lax.rsqrt(resid * resid + charb_eps2)

        each_place(receive)
        arrive(0)
        arrive(1)
        shifts = [shift_of(i) for i in range(4)]

        def forward(c, r, energy):
            block, sub = block_of(c)
            for j in range(cols):
                own = warp_ref[p, block, j, pl.ds(sub, CHUNK), :].astype(jnp.float32)
                resid_a, scaled_a = residual(0, c, r, j, own, *shifts[0])
                resid_b, scaled_b = residual(1, c, r, j, own, *shifts[1])
                energy = energy + (resid_a * scaled_a + resid_b * scaled_b)
                comb_ref[pl.ds(r, CHUNK), j * BLOCK : (j + 1) * BLOCK] = scaled_a + scaled_b
            return energy

        energy = chunk_loop(forward, jnp.zeros((CHUNK, BLOCK), jnp.float32))
        own_ref[p] = jnp.sum(energy.reshape(CHUNK // 8, 8, BLOCK), axis=0)

        def tile_copy(d):
            return remote(own_ref.at[p], tile_slots.at[p, d - 1], t_send.at[p, d - 1], t_recv.at[p, d - 1], section, lax.rem(tile + d, tiles))

        def sec_copy(d):
            return remote(sum_ref.at[p], sec_slots.at[p, d - 1], s_send.at[p, d - 1], s_recv.at[p, d - 1], lax.rem(section + d, sections), tile)

        for d in range(1, tiles):
            tile_copy(d).start()
        total = own_ref[p]
        for d in range(1, tiles):
            tile_copy(d).wait_recv()
            total = total + tile_slots[p, d - 1]
        sum_ref[p] = total
        for d in range(1, sections):
            sec_copy(d).start()
        arrive(2)
        arrive(3)
        edge_wait(u_ref.at[p], u_send.at[p], u_recv.at[p])

        def backward(c, r, carry):
            block, sub = block_of(c)
            parts = []
            for j in range(cols):
                own = warp_ref[p, block, j, pl.ds(sub, CHUNK), :].astype(jnp.float32)
                _, scaled_a = residual(2, c, r, j, own, *shifts[2])
                _, scaled_b = residual(3, c, r, j, own, *shifts[3])
                parts.append(comb_ref[pl.ds(r, CHUNK), j * BLOCK : (j + 1) * BLOCK] + (scaled_a + scaled_b))
            combined = jnp.concatenate(parts, axis=1)
            for n, grad_ref in enumerate((grow_ref, gcol_ref)):
                band = u_ref[p, n, pl.ds(r, CHUNK + 2 * PAD), :]
                here = band[PAD : PAD + CHUNK]
                left, right = left_right(here)
                around = band[PAD + 1 : PAD + 1 + CHUNK] + band[PAD - 1 : PAD - 1 + CHUNK] + (right + left)
                data_ref[n, pl.ds(r, CHUNK), :] = combined * grad_ref[pl.ds(r, CHUNK), :] + smooth_weight * (4.0 * here - around)
            return carry

        chunk_loop(backward, 0)

        each_place(finish)
        for i in range(4):
            finish_relay(i)
        total = sum_ref[p]
        for d in range(1, sections):
            sec_copy(d).wait_recv()
            total = total + sec_slots[p, d - 1]
        energy_all = jnp.sum(jnp.sum(total, axis=0, keepdims=True), axis=1, keepdims=True)
        count_all = jnp.full((1, 1), count, jnp.int32).astype(jnp.float32)
        factor = step_size / (1.0 + energy_all / count_all)
        for d in range(1, tiles):
            tile_copy(d).wait_send()
        for d in range(1, sections):
            sec_copy(d).wait_send()

        def update(c, r, carry):
            news = []
            for n in range(2):
                new = u_ref[p, n, pl.ds(r + PAD, CHUNK), :] - factor * data_ref[n, pl.ds(r, CHUNK), :]
                u_ref[1 - p, n, pl.ds(r + PAD, CHUNK), :] = new
                news.append(new)
            base = img_ref[pl.ds(r + PAD, CHUNK), :]
            store_warp(1 - p, c, base, grow_ref[pl.ds(r, CHUNK), :], gcol_ref[pl.ds(r, CHUNK), :], *news)
            return carry

        chunk_loop(update, 0)

    def two_steps(half, carry):
        step(2 * half, 0)
        step(2 * half + 1, 1)
        return carry

    lax.fori_loop(0, ITERS // 2, two_steps, 0)

    def store_out(c, r, carry):
        out_ref[0, :, pl.ds(r, CHUNK), :] = u_ref[0, :, pl.ds(r + PAD, CHUNK), :]
        return carry

    chunk_loop(store_out, 0)


def solution(mesh):
    sections, tiles = mesh.shape["sec"], mesh.shape["tile"]

    def per_device(image, field, displacement):
        rows, width = image.shape[1], image.shape[2]
        cols = width // BLOCK
        dma = pltpu.SemaphoreType.DMA
        return pl.pallas_call(
            functools.partial(kernel, sections, tiles),
            out_shape=jax.ShapeDtypeStruct(field.shape, jnp.float32),
            in_specs=[
                pl.BlockSpec(memory_space=pltpu.VMEM),
                pl.BlockSpec(memory_space=pltpu.VMEM),
                pl.BlockSpec(memory_space=pltpu.SMEM),
            ],
            out_specs=pl.BlockSpec(memory_space=pltpu.VMEM),
            scratch_shapes=[pltpu.VMEM((rows // BLOCK + 2, cols, BLOCK, BLOCK), jnp.bfloat16) for _ in range(10)]
            + [
                pltpu.VMEM((2, rows // BLOCK, cols, BLOCK, BLOCK), jnp.bfloat16),
                pltpu.VMEM((2, 2, rows + 2 * PAD, width), jnp.float32),
                pltpu.VMEM((rows + 2 * PAD, width), jnp.float32),
                pltpu.VMEM((rows, width), jnp.float32),
                pltpu.VMEM((rows, width), jnp.float32),
                pltpu.VMEM((rows, width), jnp.float32),
                pltpu.VMEM((2, rows, width), jnp.float32),
                pltpu.VMEM((2, 8, BLOCK), jnp.float32),
                pltpu.VMEM((2, 8, BLOCK), jnp.float32),
                pltpu.VMEM((2, tiles - 1, 8, BLOCK), jnp.float32),
                pltpu.VMEM((2, sections - 1, 8, BLOCK), jnp.float32),
                dma((2,)), dma((2,)),
                dma((2, 2)), dma((2, 2)),
                dma((2, 5, rows // BLOCK)), dma((2, 5, rows // BLOCK)),
                dma((2, 4, 2)), dma((2, 4, 2)),
                dma((2, 5, rows // BLOCK)),
                dma((2, tiles - 1)), dma((2, tiles - 1)),
                dma((2, sections - 1)), dma((2, sections - 1)),
            ],
            compiler_params=pltpu.CompilerParams(
                collective_id=0, has_side_effects=True, vmem_limit_bytes=48 * 1024 * 1024
            ),
        )(image, field, displacement.reshape(-1))

    return jax.shard_map(
        per_device,
        mesh=mesh,
        in_specs=(P("sec", "tile", None), P("sec", None, "tile", None), P()),
        out_specs=P("sec", None, "tile", None),
        check_vma=False,
    )
```

```python
import functools

import jax
import jax.numpy as jnp
from jax import lax
from jax.experimental import pallas as pl
from jax.experimental.pallas import tpu as pltpu
from jax.sharding import PartitionSpec as P

BLOCK = 128
ITERS = 4
CHUNK = 64
PAD = 8
OFFSETS = (1, 2, -1, -2)
EXTRA = 4

GROUP = (
    (((1, 2), (2, 3), (-4, EXTRA)), (0, 1, EXTRA), (2, 3), {0: (2, 2), 1: (4, 3), EXTRA: (3, 0)}),
    (((-1, 0), (2, 3)), (1, 2), (0, 3), {1: (4, 3)}),
    (((1, 2), (-2, 1)), (0, 3), (2, 1), {3: (-4, 1)}),
    (((-1, 0), (-2, 1), (4, EXTRA)), (2, 3, EXTRA), (0, 1), {2: (-2, 0), 3: (-4, 1), EXTRA: (-3, 2)}),
)
DIRECT = ((((-1, 0), (-2, 1), (1, 2), (2, 3)), (0, 1, 2, 3), (), {}),)

charb_eps2 = 0.25
step_size = 0.2
smooth_weight = 0.5

MESH = pl.DeviceIdType.MESH


def kernel(sections, tiles, image_ref, field_ref, disp_ref, out_ref, *scratch):
    moved_refs = (scratch[0:5], scratch[5:10])
    (warp_ref, u_ref, img_ref, grow_ref, gcol_ref, comb_ref, data_ref, own_ref, sum_ref, tile_slots, sec_slots) = scratch[10:21]
    (img_send, img_recv, u_send, u_recv, w_send, w_recv, h_send, h_recv, r_send, t_send, t_recv, s_send, s_recv) = scratch[21:]
    rows, width = grow_ref.shape
    height = rows * tiles
    cols = width // BLOCK
    chunks = rows // CHUNK
    pieces = rows // BLOCK
    plan = GROUP if sections % len(GROUP) == 0 else DIRECT
    section = lax.axis_index("sec")
    tile = lax.axis_index("tile")

    barrier = pltpu.get_barrier_semaphore()
    for d in range(1, sections):
        pl.semaphore_signal(barrier, inc=1, device_id=(lax.rem(section + d, sections), tile), device_id_type=MESH)
    for d in range(1, tiles):
        pl.semaphore_signal(barrier, inc=1, device_id=(section, lax.rem(tile + d, tiles)), device_id_type=MESH)

    def remote(src, dst, send, recv, sec_at, tile_at):
        return pltpu.make_async_remote_copy(
            src_ref=src, dst_ref=dst, send_sem=send, recv_sem=recv, device_id=(sec_at, tile_at), device_id_type=MESH
        )

    has_above = tile > 0
    has_below = tile < tiles - 1
    above = jnp.maximum(tile - 1, 0)
    below = jnp.minimum(tile + 1, tiles - 1)

    def edge_copies(ref, send, recv):
        up = remote(ref.at[..., pl.ds(PAD, PAD), :], ref.at[..., pl.ds(rows + PAD, PAD), :], send.at[0], recv.at[0], section, above)
        down = remote(ref.at[..., pl.ds(rows, PAD), :], ref.at[..., pl.ds(0, PAD), :], send.at[1], recv.at[1], section, below)
        return up, down

    def edge_start(ref, send, recv):
        up, down = edge_copies(ref, send, recv)
        pl.when(has_above)(up.start)
        pl.when(has_below)(down.start)

    def edge_wait(ref, send, recv):
        up, down = edge_copies(ref, send, recv)
        pl.when(has_below)(up.wait_recv)
        pl.when(has_above)(down.wait_recv)
        pl.when(has_above)(up.wait_send)
        pl.when(has_below)(down.wait_send)

    @pl.when(jnp.logical_not(has_above))
    def _():
        img_ref[0:PAD, :] = jnp.zeros((PAD, width), jnp.float32)
        for p in range(2):
            u_ref[p, :, 0:PAD, :] = jnp.zeros((2, PAD, width), jnp.float32)

    @pl.when(jnp.logical_not(has_below))
    def _():
        img_ref[rows + PAD : rows + 2 * PAD, :] = jnp.zeros((PAD, width), jnp.float32)
        for p in range(2):
            u_ref[p, :, rows + PAD : rows + 2 * PAD, :] = jnp.zeros((2, PAD, width), jnp.float32)

    def chunk_loop(body, init=None):
        def step(c, carry):
            return body(c, pl.multiple_of(c * CHUNK, CHUNK), carry)

        return lax.fori_loop(0, chunks, step, init)

    def load_in(c, r, carry):
        img_ref[pl.ds(r + PAD, CHUNK), :] = image_ref[0, pl.ds(r, CHUNK), :].astype(jnp.float32)
        u_ref[0, :, pl.ds(r + PAD, CHUNK), :] = field_ref[0, :, pl.ds(r, CHUNK), :]
        return carry

    chunk_loop(load_in, 0)

    pl.semaphore_wait(barrier, sections - 1 + tiles - 1)
    edge_start(img_ref, img_send, img_recv)

    def block_of(c):
        block = c // (BLOCK // CHUNK)
        return block, pl.multiple_of((c - block * (BLOCK // CHUNK)) * CHUNK, CHUNK)

    col_ids = lax.broadcasted_iota(jnp.int32, (CHUNK, width), 1)

    def left_right(x):
        left = jnp.where(col_ids == 0, 0.0, pltpu.roll(x, 1, 1))
        right = jnp.where(col_ids == width - 1, 0.0, pltpu.roll(x, width - 1, 1))
        return left, right

    def store_warp(p, c, base, grow, gcol, u0, u1):
        warped = (base + grow * u0 + gcol * u1).astype(jnp.bfloat16)
        block, sub = block_of(c)
        for j in range(cols):
            warp_ref[p, block, j, pl.ds(sub, CHUNK), :] = warped[:, j * BLOCK : (j + 1) * BLOCK]

    def first_warp(c, r, carry):
        band = img_ref[pl.ds(r, CHUNK + 2 * PAD), :]
        base = band[PAD : PAD + CHUNK]
        grow = 0.5 * (band[PAD + 1 : PAD + 1 + CHUNK] - band[PAD - 1 : PAD - 1 + CHUNK])
        left, right = left_right(base)
        gcol = 0.5 * (right - left)
        grow_ref[pl.ds(r, CHUNK), :] = grow
        gcol_ref[pl.ds(r, CHUNK), :] = gcol
        u0 = u_ref[0, 0, pl.ds(r + PAD, CHUNK), :]
        u1 = u_ref[0, 1, pl.ds(r + PAD, CHUNK), :]
        store_warp(0, c, base, grow, gcol, u0, u1)
        return carry

    def inner_warp(c, carry):
        return first_warp(c, pl.multiple_of(c * CHUNK, CHUNK), carry)

    lax.fori_loop(1, chunks - 1, inner_warp, 0)
    edge_wait(img_ref, img_send, img_recv)
    first_warp(0, 0, 0)
    first_warp(chunks - 1, rows - CHUNK, 0)

    def in_stack(at):
        return (at >= 0) & (at < sections)

    def step(turn, p):
        refs = moved_refs[p]

        def source_of(place, i):
            return OFFSETS[i] if i != EXTRA else (4 if place == 0 else -4)

        def piece_copy(src, slot, q, send, offset):
            target = jnp.minimum(jnp.maximum(section + offset, 0), sections - 1)
            return remote(src, refs[slot].at[1 + q], send, w_recv.at[p, slot, q], target, tile)

        def own_copy(offset, slot, q):
            return piece_copy(warp_ref.at[p, q], slot, q, w_send.at[p, slot, q], offset)

        def pass_copy(i, offset, slot, q):
            return piece_copy(refs[i].at[1 + q], slot, q, r_send.at[p, i, q], offset)

        def relay_up(i):
            return remote(
                refs[i].at[1], refs[i].at[rows // BLOCK + 1],
                h_send.at[p, i, 0], h_recv.at[p, i, 0], section, above,
            )

        def relay_down(i):
            return remote(
                refs[i].at[rows // BLOCK], refs[i].at[0],
                h_send.at[p, i, 1], h_recv.at[p, i, 1], section, below,
            )

        def start_own(place):
            for q in range(pieces):
                for offset, slot in plan[place][0]:
                    pl.when(in_stack(section + offset))(own_copy(offset, slot, q).start)

        def receive(place):
            _, near, far, passes = plan[place]
            for slots in (near, far):
                for q in range(pieces):
                    for i in slots:

                        @pl.when(in_stack(section + source_of(place, i)))
                        def _():
                            own_copy(0, i, q).wait_recv()
                            if i in passes:
                                offset, slot = passes[i]
                                pl.when(in_stack(section + offset))(pass_copy(i, offset, slot, q).start)
                            if i != EXTRA and q == 0:
                                pl.when(has_above)(relay_up(i).start)
                            if i != EXTRA and q == pieces - 1:
                                pl.when(has_below)(relay_down(i).start)

        def arrive(i):
            @pl.when(in_stack(section + OFFSETS[i]))
            def _():
                pl.when(has_below)(relay_up(i).wait_recv)
                pl.when(has_above)(relay_down(i).wait_recv)

        def finish(place):
            own, _, _, passes = plan[place]
            for q in range(pieces):
                for offset, slot in own:
                    pl.when(in_stack(section + offset))(own_copy(offset, slot, q).wait_send)
                for i, (offset, slot) in passes.items():
                    has_both = in_stack(section + source_of(place, i)) & in_stack(section + offset)
                    pl.when(has_both)(pass_copy(i, offset, slot, q).wait_send)

        def finish_relay(i):
            @pl.when(in_stack(section + OFFSETS[i]))
            def _():
                pl.when(has_above)(relay_up(i).wait_send)
                pl.when(has_below)(relay_down(i).wait_send)

        def each_place(action):
            for place in range(len(plan)):
                pl.when(lax.rem(section, len(plan)) == place)(functools.partial(action, place))

        each_place(start_own)
        edge_start(u_ref.at[p], u_send.at[p], u_recv.at[p])

        def count_one(s, total):
            for g in (1, 2):
                at = ((turn * sections + s) * 2 + (g - 1)) * 2
                area = (height - BLOCK * jnp.abs(disp_ref[at])) * (width - BLOCK * jnp.abs(disp_ref[at + 1]))
                total = total + (s + g < sections).astype(jnp.int32) * area
            return total

        count = lax.fori_loop(0, sections, count_one, jnp.int32(0))

        def shift_of(i):
            g = abs(OFFSETS[i])
            first = section if OFFSETS[i] > 0 else jnp.maximum(section - g, 0)
            sign = 1 if OFFSETS[i] > 0 else -1
            at = ((turn * sections + first) * 2 + (g - 1)) * 2
            return sign * disp_ref[at], sign * disp_ref[at + 1]

        def residual(i, c, r, j, own, down, across):
            block, sub = block_of(c)
            row_block = tile * (rows // BLOCK) + block + down
            col_block = j + across
            good = in_stack(section + OFFSETS[i]) & (row_block >= 0) & (row_block < height // BLOCK)
            good = good & (col_block >= 0) & (col_block < cols)
            other = refs[i][block + 1 + down, jnp.minimum(jnp.maximum(col_block, 0), cols - 1), pl.ds(sub, CHUNK), :].astype(jnp.float32)
            mask = jnp.full((CHUNK, BLOCK), good.astype(jnp.int32), jnp.int32)
            resid = jnp.where(mask > 0, own - other, 0.0)
            return resid, resid * lax.rsqrt(resid * resid + charb_eps2)

        each_place(receive)
        arrive(0)
        arrive(1)
        shifts = [shift_of(i) for i in range(4)]

        def forward(c, r, energy):
            block, sub = block_of(c)
            for j in range(cols):
                own = warp_ref[p, block, j, pl.ds(sub, CHUNK), :].astype(jnp.float32)
                resid_a, scaled_a = residual(0, c, r, j, own, *shifts[0])
                resid_b, scaled_b = residual(1, c, r, j, own, *shifts[1])
                energy = energy + (resid_a * scaled_a + resid_b * scaled_b)
                comb_ref[pl.ds(r, CHUNK), j * BLOCK : (j + 1) * BLOCK] = scaled_a + scaled_b
            return energy

        energy = chunk_loop(forward, jnp.zeros((CHUNK, BLOCK), jnp.float32))
        own_ref[p] = jnp.sum(energy.reshape(CHUNK // 8, 8, BLOCK), axis=0)

        def tile_copy(d):
            return remote(own_ref.at[p], tile_slots.at[p, d - 1], t_send.at[p, d - 1], t_recv.at[p, d - 1], section, lax.rem(tile + d, tiles))

        def sec_copy(d):
            return remote(sum_ref.at[p], sec_slots.at[p, d - 1], s_send.at[p, d - 1], s_recv.at[p, d - 1], lax.rem(section + d, sections), tile)

        for d in range(1, tiles):
            tile_copy(d).start()
        total = own_ref[p]
        for d in range(1, tiles):
            tile_copy(d).wait_recv()
            total = total + tile_slots[p, d - 1]
        sum_ref[p] = total
        for d in range(1, sections):
            sec_copy(d).start()
        arrive(2)
        arrive(3)
        edge_wait(u_ref.at[p], u_send.at[p], u_recv.at[p])

        def backward(c, r, carry):
            block, sub = block_of(c)
            parts = []
            for j in range(cols):
                own = warp_ref[p, block, j, pl.ds(sub, CHUNK), :].astype(jnp.float32)
                _, scaled_a = residual(2, c, r, j, own, *shifts[2])
                _, scaled_b = residual(3, c, r, j, own, *shifts[3])
                parts.append(comb_ref[pl.ds(r, CHUNK), j * BLOCK : (j + 1) * BLOCK] + (scaled_a + scaled_b))
            combined = jnp.concatenate(parts, axis=1)
            for n, grad_ref in enumerate((grow_ref, gcol_ref)):
                band = u_ref[p, n, pl.ds(r, CHUNK + 2 * PAD), :]
                here = band[PAD : PAD + CHUNK]
                left, right = left_right(here)
                around = band[PAD + 1 : PAD + 1 + CHUNK] + band[PAD - 1 : PAD - 1 + CHUNK] + (right + left)
                data_ref[n, pl.ds(r, CHUNK), :] = combined * grad_ref[pl.ds(r, CHUNK), :] + smooth_weight * (4.0 * here - around)
            return carry

        chunk_loop(backward, 0)

        each_place(finish)
        for i in range(4):
            finish_relay(i)
        total = sum_ref[p]
        for d in range(1, sections):
            sec_copy(d).wait_recv()
            total = total + sec_slots[p, d - 1]
        energy_all = jnp.sum(jnp.sum(total, axis=0, keepdims=True), axis=1, keepdims=True)
        count_all = jnp.full((1, 1), count, jnp.int32).astype(jnp.float32)
        factor = step_size / (1.0 + energy_all / count_all)
        for d in range(1, tiles):
            tile_copy(d).wait_send()
        for d in range(1, sections):
            sec_copy(d).wait_send()

        def update(c, r, carry):
            news = []
            for n in range(2):
                new = u_ref[p, n, pl.ds(r + PAD, CHUNK), :] - factor * data_ref[n, pl.ds(r, CHUNK), :]
                u_ref[1 - p, n, pl.ds(r + PAD, CHUNK), :] = new
                news.append(new)
            base = img_ref[pl.ds(r + PAD, CHUNK), :]
            store_warp(1 - p, c, base, grow_ref[pl.ds(r, CHUNK), :], gcol_ref[pl.ds(r, CHUNK), :], *news)
            return carry

        chunk_loop(update, 0)

    def two_steps(half, carry):
        step(2 * half, 0)
        step(2 * half + 1, 1)
        return carry

    lax.fori_loop(0, ITERS // 2, two_steps, 0)

    def store_out(c, r, carry):
        out_ref[0, :, pl.ds(r, CHUNK), :] = u_ref[0, :, pl.ds(r + PAD, CHUNK), :]
        return carry

    chunk_loop(store_out, 0)


def solution(mesh):
    sections, tiles = mesh.shape["sec"], mesh.shape["tile"]

    def per_device(image, field, displacement):
        rows, width = image.shape[1], image.shape[2]
        cols = width // BLOCK
        dma = pltpu.SemaphoreType.DMA
        return pl.pallas_call(
            functools.partial(kernel, sections, tiles),
            out_shape=jax.ShapeDtypeStruct(field.shape, jnp.float32),
            in_specs=[
                pl.BlockSpec(memory_space=pltpu.VMEM),
                pl.BlockSpec(memory_space=pltpu.VMEM),
                pl.BlockSpec(memory_space=pltpu.SMEM),
            ],
            out_specs=pl.BlockSpec(memory_space=pltpu.VMEM),
            scratch_shapes=[pltpu.VMEM((rows // BLOCK + 2, cols, BLOCK, BLOCK), jnp.bfloat16) for _ in range(10)]
            + [
                pltpu.VMEM((2, rows // BLOCK, cols, BLOCK, BLOCK), jnp.bfloat16),
                pltpu.VMEM((2, 2, rows + 2 * PAD, width), jnp.float32),
                pltpu.VMEM((rows + 2 * PAD, width), jnp.float32),
                pltpu.VMEM((rows, width), jnp.float32),
                pltpu.VMEM((rows, width), jnp.float32),
                pltpu.VMEM((rows, width), jnp.float32),
                pltpu.VMEM((2, rows, width), jnp.float32),
                pltpu.VMEM((2, 8, BLOCK), jnp.float32),
                pltpu.VMEM((2, 8, BLOCK), jnp.float32),
                pltpu.VMEM((2, tiles - 1, 8, BLOCK), jnp.float32),
                pltpu.VMEM((2, sections - 1, 8, BLOCK), jnp.float32),
                dma((2,)), dma((2,)),
                dma((2, 2)), dma((2, 2)),
                dma((2, 5, rows // BLOCK)), dma((2, 5, rows // BLOCK)),
                dma((2, 4, 2)), dma((2, 4, 2)),
                dma((2, 5, rows // BLOCK)),
                dma((2, tiles - 1)), dma((2, tiles - 1)),
                dma((2, sections - 1)), dma((2, sections - 1)),
            ],
            compiler_params=pltpu.CompilerParams(
                collective_id=0, has_side_effects=True, vmem_limit_bytes=48 * 1024 * 1024
            ),
        )(image, field, displacement.reshape(-1))

    return jax.shard_map(
        per_device,
        mesh=mesh,
        in_specs=(P("sec", "tile", None), P("sec", None, "tile", None), P()),
        out_specs=P("sec", None, "tile", None),
        check_vma=False,
    )
```
